256 devices in a mesh: task: 8 (over z), shard: 8 (over y, core), rep: 4 (over x).
Axes of the slice: x: 4, y: 4, z: 8, core: 2. Of those that a mesh axis runs over, the one named last changes fastest.
Arguments:
- deltas: bfloat16 [16, 256, 16, 8192], P('task', None, None, ('shard', 'rep')), may hold values from -4 to 4
- base: bfloat16 [256, 16, 8, 1024], P(('task', 'shard'), None, None, 'rep'), may hold values from -60 to 60
- sel_index: int32 [16, 64], replicated, may hold values from 0 to 255, as said below
- sel_count: int32 [16], replicated, may hold values from 1 to 64
- scale_num: int32 [16], replicated, may hold values from 1 to 12
Outputs:
- merged: bfloat16 [256, 16, 8192], P(('task', 'shard'))
The draws below stay inside these ranges and needn't reach their ends.
Inputs may be any that keep to these rules, and one draw needn't show every extreme that they name: `sel_index`: for task i the first sel_count[i] entries are distinct and ascending; at most 1 of them lie in any aligned group of 4 blocks, and in every draw some group holds 1 selected blocks of every task, and some task selects 1 block in every group. Later entries are block numbers that are not selected.
All inputs are finite; a program needn't handle non-finite values.
Results may differ from the reference program's by a relative error of at most 0.00045.
Values may be sent and summed in bfloat16 or wider, within the bound.
No kernel may reach another device: no remote copies, remote signals or barrier semaphores. Data moves between devices by JAX's collectives and lax.ppermute only.
A program may use at most 64 MiB of HBM per device.

```python
import jax
import jax.numpy as jnp
from jax import lax

D = 8192
LAYERS = 4
BR = 16
OB = 4
CAP = 1
OWNERS = 64
NB_ALL = 256
KMAX = 64
TASKS = 16
N_SHARD = 8


def pick_blocks(key):
    inner = jax.random.fold_in(key, 11)
    keys = jax.random.split(inner, 5)
    counts = jax.random.randint(keys[0], (TASKS, OWNERS), 0, CAP + 1)
    common = jax.random.randint(keys[1], (), 0, OWNERS)
    single = jax.random.randint(keys[2], (TASKS,), 0, OWNERS)
    full_task = jax.random.randint(keys[4], (), 0, TASKS)
    owner_ids = jnp.arange(OWNERS, dtype=jnp.int32)
    task_ids = jnp.arange(TASKS, dtype=jnp.int32)
    filled = (owner_ids[None, :] == common) | (owner_ids[None, :] == single[:, None]) | (task_ids[:, None] == full_task)
    counts = jnp.where(filled, CAP, counts)
    scores = jax.random.randint(keys[3], (TASKS, OWNERS, OB), 0, 1 << 20) * OB + jnp.arange(OB, dtype=jnp.int32)
    order = jnp.argsort(scores, axis=-1)
    ranks = jnp.argsort(order, axis=-1)
    chosen = (ranks < counts[:, :, None]).reshape(TASKS, NB_ALL)
    blocks = jnp.arange(NB_ALL, dtype=jnp.int32)
    sort_key = jnp.where(chosen, blocks[None, :], NB_ALL + blocks[None, :])
    listed = jnp.argsort(sort_key, axis=1)[:, :KMAX].astype(jnp.int32)
    total = jnp.sum(chosen.astype(jnp.int32), axis=1).astype(jnp.int32)
    return (listed, total)


def draw_sel_index(key, part):
    return pick_blocks(key)[0]


def draw_sel_count(key, part):
    return pick_blocks(key)[1]


def base_values(key):
    keys = jax.random.split(jax.random.fold_in(key, 5), 2)
    group_cols = D // N_SHARD
    shape = (NB_ALL, BR, N_SHARD, group_cols)
    block_rise = 0.6 * jnp.exp(jnp.log(3.0) * jnp.arange(NB_ALL, dtype=jnp.float32) / max(NB_ALL - 1, 1))
    col_rise = 0.6 * jnp.exp(jnp.log(3.0) * jnp.arange(group_cols, dtype=jnp.float32) / max(group_cols - 1, 1))
    noise = jnp.clip(jax.random.normal(keys[0], shape, jnp.float32), -6.0, 6.0)
    row_scale = jnp.exp(jax.random.uniform(keys[1], (NB_ALL, BR), jnp.float32, jnp.log(0.5), jnp.log(2.0)))
    values = noise * block_rise[:, None, None, None] * row_scale[:, :, None, None]
    values = values * col_rise[None, None, None, :]
    return values


def draw_base(key, part):
    return base_values(key).astype(jnp.bfloat16)


def draw_deltas(key, part):
    keys = jax.random.split(jax.random.fold_in(key, 23), 2)
    shaped = base_values(key).reshape(NB_ALL, BR, D)
    noise = 0.45 * jnp.clip(jax.random.normal(keys[0], (TASKS, NB_ALL, BR, D), jnp.float32), -6.0, 6.0)
    shared = 0.3 * jnp.clip(jax.random.normal(keys[1], (NB_ALL, BR, D), jnp.float32), -6.0, 6.0)
    tie = 0.04
    values = noise + shared[None] + tie * shaped[None]
    return jnp.clip(values, -4.0, 4.0).astype(jnp.bfloat16)


def place_ends(drawn, key, least, top_value):
    extent = drawn.shape
    spot = [jax.random.randint(jax.random.fold_in(key, axis), (), 0, extent[axis]) for axis in range(len(extent))]
    drawn = drawn.at[tuple(spot)].set(least)
    longest = extent.index(max(extent))
    spot[longest] = (spot[longest] + 1) % extent[longest]
    return drawn.at[tuple(spot)].set(top_value)


def setup_inputs(seed: int = 0) -> dict:
    seeds = jax.random.split(jax.random.key(seed), 6)
    return {
        "deltas": draw_deltas(jax.random.fold_in(seeds[5], 71), 0),
        "base": draw_base(jax.random.fold_in(seeds[5], 71), 0),
        "sel_index": draw_sel_index(jax.random.fold_in(seeds[5], 71), 0),
        "sel_count": draw_sel_count(jax.random.fold_in(seeds[5], 71), 0),
        "scale_num": place_ends(jax.random.randint(seeds[4], (TASKS,), 1, 13), jax.random.fold_in(seeds[4], 1), 1, 12).astype(jnp.int32),
    }


denominator = 8.0
epsilon = 1e-06

def reference(deltas, base, sel_index, sel_count, scale_num):
    entries = jnp.arange(KMAX, dtype=jnp.int32)
    valid = entries[None, :] < sel_count[:, None]
    blocks = jnp.arange(NB_ALL, dtype=jnp.int32)
    hits = (sel_index[:, :, None] == blocks[None, None, :]) & valid[:, :, None]
    picked = lax.optimization_barrier(jnp.sum(hits.astype(jnp.float32), axis=1))
    weight = picked * (scale_num.astype(jnp.float32) / denominator)[:, None]

    def accumulate(total, item):
        delta, factor = item
        return (total + factor[:, None, None] * delta.astype(jnp.float32), None)
    combined, _ = lax.scan(accumulate, jnp.zeros((NB_ALL, BR, D), jnp.float32), (deltas, weight))
    base_full = base.reshape(NB_ALL, BR, D).astype(jnp.float32)
    merged_raw = base_full + combined
    span = NB_ALL // LAYERS
    base_sq = lax.optimization_barrier(jnp.sum(lax.optimization_barrier(jnp.sum(base_full * base_full, axis=(1, 2))).reshape(LAYERS, span), axis=1))
    merged_sq = lax.optimization_barrier(jnp.sum(lax.optimization_barrier(jnp.sum(merged_raw * merged_raw, axis=(1, 2))).reshape(LAYERS, span), axis=1))
    ratio = jnp.sqrt((base_sq + epsilon) / (merged_sq + epsilon))
    per_block = ratio[blocks // span]
    return (merged_raw * per_block[:, None, None]).astype(jnp.bfloat16)
```

```python
import functools

import jax
import jax.numpy as jnp
from jax import lax
from jax.experimental import pallas as pl
from jax.experimental.pallas import tpu as pltpu
from jax.sharding import Mesh
from jax.sharding import PartitionSpec as P

TASK = ("layer", "half")
SHARD = ("shard_0", "shard_1")
OWNER = ("layer", "half", "shard_0", "shard_1")
SAME_LAYER = ("half", "shard_0", "shard_1", "rep")
LAYERS = 4
DENOMINATOR = 8.0
EPSILON = 1e-06
LANES = 128


KERNEL = pltpu.CompilerParams(vmem_limit_bytes=16 * 2**20)


def cost(flops, bytes_accessed):
    return pl.CostEstimate(flops=flops, bytes_accessed=bytes_accessed, transcendentals=0)


def pick_kernel(own, sel_ref, count_ref, deltas_ref, out_ref, table, sem):
    owners, task_dev = out_ref.shape[:2]
    first = lax.axis_index(TASK) * task_dev
    entries = sel_ref.shape[1]

    def start_row(o, carry):
        for a in range(task_dev):
            table[a, o] = o * own
        return carry

    lax.fori_loop(0, owners, start_row, 0, unroll=8)

    for a in range(task_dev):
        count = count_ref[first + a]

        def note(k, carry, a=a):
            block = sel_ref[first + a, k]
            table[a, block // own] = block
            return carry

        lax.fori_loop(0, count, note, 0)

    def copy_row(o, carry):
        for a in range(task_dev):
            pltpu.make_async_copy(deltas_ref.at[a, table[a, o]], out_ref.at[o, a], sem).start()
        return carry

    lax.fori_loop(0, owners, copy_row, 0, unroll=4)
    pltpu.make_async_copy(out_ref, out_ref, sem).wait()


def pick(sel_index, sel_count, deltas, owners, own):
    task_dev, _, rows, width = deltas.shape
    smem = pl.BlockSpec(memory_space=pltpu.SMEM)
    return pl.pallas_call(
        functools.partial(pick_kernel, own),
        out_shape=jax.ShapeDtypeStruct((owners, task_dev, rows, width), deltas.dtype),
        in_specs=[smem, smem, pl.BlockSpec(memory_space=pl.ANY)],
        out_specs=pl.BlockSpec(memory_space=pltpu.VMEM),
        scratch_shapes=[pltpu.SMEM((task_dev, owners), jnp.int32), pltpu.SemaphoreType.DMA],
        cost_estimate=cost(10_000_000, 2 * owners * task_dev * rows * width * 2),
        name="pick",
    )(sel_index, sel_count, deltas)


def combine_kernel(incoming_ref, base_ref, weight_ref, merged_ref, sums_ref):
    n_task, groups, task_dev, rows, width = incoming_ref.shape
    own = base_ref.shape[0]

    def group(s, sums):
        base_sum, merged_sum = sums
        total = [base_ref[j, s].astype(jnp.float32) for j in range(own)]
        for j in range(own):
            base_sum = base_sum + jnp.sum(total[j] * total[j], axis=0, keepdims=True)
        for t in range(n_task):
            for a in range(task_dev):
                delta = incoming_ref[t, s, a].astype(jnp.float32)
                for j in range(own):
                    total[j] = total[j] + weight_ref[j, t * task_dev + a : t * task_dev + a + 1] * delta
        for j in range(own):
            merged_ref[j, s] = total[j]
            merged_sum = merged_sum + jnp.sum(total[j] * total[j], axis=0, keepdims=True)
        return base_sum, merged_sum

    zero = jnp.zeros((1, width), jnp.float32)
    base_sum, merged_sum = lax.fori_loop(0, groups, group, (zero, zero))
    fold = lambda row: functools.reduce(jnp.add, [row[:, k : k + LANES] for k in range(0, width, LANES)])
    sums_ref[0:1] = fold(base_sum)
    sums_ref[1:2] = fold(merged_sum)


def combine(incoming, base, weight):
    vmem = pl.BlockSpec(memory_space=pltpu.VMEM)
    return pl.pallas_call(
        combine_kernel,
        out_shape=[
            jax.ShapeDtypeStruct(base.shape, jnp.float32),
            jax.ShapeDtypeStruct((2, LANES), jnp.float32),
        ],
        in_specs=[vmem] * 3,
        out_specs=[vmem] * 2,
        compiler_params=KERNEL,
        cost_estimate=cost(3_000_000, 3_000_000),
        name="combine",
    )(incoming, base, weight)


def scale_kernel(merged_ref, sums_ref, out_ref):
    ratio = ratio_of(sums_ref)
    for j in range(merged_ref.shape[0]):
        out_ref[j] = (merged_ref[j] * ratio).astype(out_ref.dtype)


def ratio_of(sums_ref):
    total = jnp.sum(sums_ref[...], axis=0)
    base_sq = jnp.sum(total[0:1], axis=1, keepdims=True)
    merged_sq = jnp.sum(total[1:2], axis=1, keepdims=True)
    return jnp.sqrt((base_sq + EPSILON) / (merged_sq + EPSILON))[None]


def scale(merged, sums):
    vmem = pl.BlockSpec(memory_space=pltpu.VMEM)
    return pl.pallas_call(
        scale_kernel,
        out_shape=jax.ShapeDtypeStruct(merged.shape, jnp.bfloat16),
        in_specs=[vmem] * 2,
        out_specs=vmem,
        compiler_params=KERNEL,
        cost_estimate=cost(1_000_000, 1_000_000),
        name="scale",
    )(merged, sums)


def lay_kernel(parts_ref, out_ref):
    reps, own, groups, rows, width = parts_ref.shape
    for r in range(reps):
        for s in range(groups):
            at = (s * reps + r) * width
            out_ref[:, :, at : at + width] = parts_ref[r, :, s]


def lay(parts):
    reps, own, groups, rows, width = parts.shape
    return pl.pallas_call(
        lay_kernel,
        out_shape=jax.ShapeDtypeStruct((own, rows, groups * reps * width), parts.dtype),
        in_specs=[pl.BlockSpec(memory_space=pltpu.VMEM)],
        out_specs=pl.BlockSpec(memory_space=pltpu.VMEM),
        compiler_params=KERNEL,
        cost_estimate=cost(1_000_000, 2_000_000),
        name="lay",
    )(parts)


def sent_to_all(value, axes):
    copies = jnp.broadcast_to(value, (lax.axis_size(axes), *value.shape))
    return lax.all_to_all(copies, axes, split_axis=0, concat_axis=0, tiled=True)


def weights(sel_index, sel_count, scale_num, owner, own, width):
    entries = jnp.arange(sel_index.shape[1], dtype=jnp.int32)
    mine = (entries[None, :] < sel_count[:, None]) & (sel_index // own == owner)
    local = jnp.arange(own, dtype=jnp.int32)
    hit = jnp.any(mine[None] & ((sel_index % own)[None] == local[:, None, None]), axis=2)
    weight = jnp.where(hit, (scale_num.astype(jnp.float32) / DENOMINATOR)[None], 0.0)
    return jnp.broadcast_to(weight[:, :, None], (*weight.shape, width))


def shards(deltas, base, sel_index, sel_count, scale_num):
    task_dev, _, rows, width = deltas.shape
    n_task, n_shard = lax.axis_size(TASK), lax.axis_size(SHARD)
    owners, own = n_task * n_shard, base.shape[0]
    owner = lax.axis_index(OWNER)
    outgoing = pick(sel_index, sel_count, deltas, owners, own)
    incoming = lax.all_to_all(outgoing, OWNER, split_axis=0, concat_axis=0, tiled=True)
    weight = weights(sel_index, sel_count, scale_num, owner, own, width)
    base = jnp.swapaxes(base, 1, 2)
    incoming = incoming.reshape(n_task, n_shard, task_dev, rows, width)
    merged, sums = combine(incoming, base, weight)
    sums = sent_to_all(sums, SAME_LAYER)
    result = scale(merged, sums)
    return lay(sent_to_all(result, "rep"))


def solution(mesh):
    torus = Mesh(
        mesh.devices.reshape(LAYERS, mesh.shape["task"] // LAYERS, mesh.shape["shard"] // 2, 2, mesh.shape["rep"]),
        ("layer", "half", "shard_0", "shard_1", "rep"),
    )
    placed = (P(TASK, None, None, (*SHARD, "rep")), P(OWNER, None, None, "rep"), P(), P(), P())
    return jax.shard_map(shards, mesh=torus, in_specs=placed, out_specs=P(OWNER, None, None), check_vma=False)
```
